32 devices in a mesh: seq: 4 (over y, x), tp: 8 (over z, core).
Axes of the slice: x: 2, y: 2, z: 4, core: 2. Of those that a mesh axis runs over, the one named last changes fastest.
Arguments:
- tokens: bfloat16 [1, 512, 4096], P(None, 'seq', 'tp'), may hold values from -6 to 6
- projections: bfloat16 [4096, 3, 4096], P(None, None, 'tp'), may hold values from -1.5 to 1.5
- out_weight: bfloat16 [4096, 4096], P('tp'), may hold values from -0.09375 to 0.09375
- gain_in: float32 [4096], P('tp'), may hold values from 0.5 to 1.5
- gain_out: float32 [4096], P('tp'), may hold values from 0.5 to 1.5
- iterates: float32 [5, 1, 512, 4096], P(None, None, 'seq', 'tp'), may hold values from -5 to 5
- images: float32 [5, 1, 512, 4096], P(None, None, 'seq', 'tp'), may hold values from -330 to 330
Outputs:
- mixed: float32 [1, 512, 4096], P(None, 'seq', 'tp')
- image: float32 [1, 512, 4096], P(None, 'seq', 'tp')
The draws below stay inside these ranges and needn't reach their ends.
All inputs are finite; a program needn't handle non-finite values.
Results may differ from the reference program's by a relative error of at most 0.013.
Values may be sent and summed in bfloat16 or wider, within the bound.
A program may use at most 64 MiB of HBM per device.

```python
import jax
import jax.numpy as jnp
from jax import lax

D = 4096
H = 32
HEAD_SIZE = 128
MEM = 5
ITERS = 2
BATCH = 1
SEQ = 512


scale_blocks = 16


def draw_projections(key, part):
    first_key = jax.random.fold_in(key, 0)
    base = jnp.clip(jax.random.normal(first_key, (D, 3, H * HEAD_SIZE), jnp.float32), -6.0, 6.0) * D ** (-0.5)
    return jnp.clip(base, -1.5, 1.5).astype(jnp.bfloat16)


def history_parts(key):
    inner = jax.random.fold_in(key, 7)
    token_key, base_key, common_key, noise_key, mixing_key, block_key = jax.random.split(inner, 6)
    field_shape = (BATCH, SEQ, D)
    shape = (MEM, BATCH, SEQ, D)
    token_part = jnp.clip(jax.random.normal(token_key, field_shape, jnp.float32), -6.0, 6.0)
    base = jnp.clip(jax.random.normal(base_key, shape, jnp.float32), -5.0, 5.0)
    common = jnp.clip(jax.random.normal(common_key, (3,) + field_shape, jnp.float32), -5.0, 5.0)
    noise_weight = 0.5
    noise = jnp.clip(jax.random.normal(noise_key, shape, jnp.float32), -5.0, 5.0)
    components = jnp.concatenate([token_part[None], common], axis=0)
    mixing = jnp.clip(0.5 * jax.random.normal(mixing_key, (MEM, 4), jnp.float32), -1.0, 1.0)
    shared = jnp.einsum('mk,kbsd->mbsd', mixing, components, precision=lax.Precision.HIGHEST)
    scale_table = jnp.exp(jax.random.uniform(block_key, (MEM, scale_blocks, scale_blocks), jnp.float32, -1.5, 1.5))
    seq_block = jnp.arange(SEQ, dtype=jnp.int32) * scale_blocks // SEQ
    feature_block = jnp.arange(D, dtype=jnp.int32) * scale_blocks // D
    block_scale = scale_table[:, seq_block, :][:, :, feature_block]
    level = 0.25 * 2.0 ** ((MEM - 1 - jnp.arange(MEM).astype(jnp.float32)) / 2.0)
    ramp = 1.0 + 2.0 * jnp.arange(SEQ).astype(jnp.float32) / max(SEQ - 1, 1)
    weighting = level[:, None, None] * ramp[None, :, None] * block_scale
    residual = (shared + noise_weight * noise) * weighting[:, None]
    return (token_part, base, base + residual)


def draw_tokens(key, part):
    return history_parts(key)[0].astype(jnp.bfloat16)


def draw_iterates(key, part):
    return history_parts(key)[1]


def draw_images(key, part):
    return history_parts(key)[2]


def levels(rng, shape, shards, smallest, high):
    loudness = 1.0
    for dim, blocks in shards:
        heights = jax.random.uniform(jax.random.fold_in(jax.random.fold_in(rng, 6), dim), (blocks,), jnp.float32, smallest / len(shards), high / len(shards))
        loudness = loudness * jnp.repeat(jnp.exp(heights), shape[dim] // blocks).reshape((-1,) + (1,) * (len(shape) - 1 - dim))
    return loudness


def scatter_about(stream_key, shape, deviation, reach, cuts=(), kind=jnp.bfloat16):
    gain = levels(stream_key, shape, cuts, -0.22, 0.18) if cuts else 1.0
    drawn = jax.random.normal(stream_key, shape, jnp.float32) * deviation * gain
    return jnp.minimum(jnp.maximum(drawn, -reach), reach).astype(kind)


def setup_inputs(seed: int = 0) -> dict:
    key_of = jax.random.split(jax.random.key(seed), 8)
    return {
        "tokens": draw_tokens(jax.random.fold_in(key_of[7], 71), 0),
        "projections": draw_projections(jax.random.fold_in(key_of[7], 71), 0),
        "out_weight": scatter_about(key_of[2], (H * HEAD_SIZE, D), (H * HEAD_SIZE) ** -0.5, 0.09375, ((0, 8),)),
        "gain_in": jnp.clip(1.0 + 0.1 * jax.random.normal(key_of[3], (D,), jnp.float32), 0.5, 1.5),
        "gain_out": jnp.clip(1.0 + 0.1 * jax.random.normal(key_of[4], (D,), jnp.float32), 0.5, 1.5),
        "iterates": draw_iterates(jax.random.fold_in(key_of[7], 71), 0),
        "images": draw_images(jax.random.fold_in(key_of[7], 71), 0),
    }


epsilon = 1e-05
rope_base = 10000.0
ridge_factor = 0.01

def inverse_rms(value_rows):
    return lax.rsqrt(lax.optimization_barrier(jnp.mean(value_rows * value_rows, axis=-1, keepdims=True)) + epsilon)

def rotate(vectors, positions):
    half_dim = vectors.shape[-1] // 2
    frequency = rope_base ** (-2.0 * jnp.arange(half_dim).astype(jnp.float32) / vectors.shape[-1])
    angles = positions[:, None] * frequency[None, :]
    cosine = jnp.cos(angles)
    sine_part = jnp.sin(angles)
    first_half = vectors[..., :half_dim]
    second_half = vectors[..., half_dim:]
    return jnp.concatenate([first_half * cosine - second_half * sine_part, second_half * cosine + first_half * sine_part], axis=-1)

def solve_small(matrix, target):
    extent = matrix.shape[0]
    indices = jnp.arange(extent)
    for column in range(extent):
        factor = jnp.where(indices > column, matrix[:, column] / matrix[column, column], 0.0)
        matrix = matrix - factor[:, None] * matrix[column][None, :]
        target = target - factor * target[column]
    answer = jnp.zeros_like(target)
    for column in reversed(range(extent)):
        entry_value = (target[column] - jnp.sum(matrix[column] * answer)) / matrix[column, column]
        answer = answer.at[column].set(entry_value)
    return answer

def anderson_weights(gram):
    extent = gram.shape[0]
    ridge = ridge_factor * jnp.trace(gram) / extent
    regular = gram + ridge * jnp.eye(extent, dtype=gram.dtype)
    solved = solve_small(regular, jnp.ones((extent,), gram.dtype))
    return solved / jnp.sum(solved)

def attend_head(operands):
    query_rows, key_rows, value_rows = operands
    length = query_rows.shape[1]
    logit_scores = jnp.einsum('oir,osr->ois', query_rows.astype(jnp.float32), key_rows.astype(jnp.float32), precision=lax.Precision.HIGHEST) * HEAD_SIZE ** (-0.5)
    causal = jnp.arange(length)[None, :] <= jnp.arange(length)[:, None]
    logit_scores = jnp.where(causal[None], logit_scores, -1e+30)
    highest = lax.optimization_barrier(jnp.max(logit_scores, axis=-1, keepdims=True))
    softmax_weights = jnp.where(causal[None], jnp.exp(logit_scores - highest), 0.0)
    total = lax.optimization_barrier(jnp.sum(softmax_weights, axis=-1, keepdims=True))
    value_mixture = jnp.einsum('atf,afv->atv', softmax_weights.astype(jnp.bfloat16).astype(jnp.float32), value_rows.astype(jnp.float32), precision=lax.Precision.HIGHEST)
    return (value_mixture / total).astype(jnp.bfloat16)

def layer_map(field, tokens, projections, out_weight, gain_in, gain_out):
    batch_count, length, width = field.shape
    heads = projections.shape[2] // HEAD_SIZE
    normed = (field * inverse_rms(field) * gain_in).astype(jnp.bfloat16)
    mapped = jnp.einsum('bsd,dce->bsce', normed.astype(jnp.float32), projections.astype(jnp.float32), precision=lax.Precision.HIGHEST)
    pieces = mapped.reshape(batch_count, length, 3, heads, HEAD_SIZE).transpose(2, 3, 0, 1, 4)
    positions = jnp.arange(length).astype(jnp.float32)
    query_rows = rotate(pieces[0], positions).astype(jnp.bfloat16)
    key_rows = rotate(pieces[1], positions).astype(jnp.bfloat16)
    value_rows = pieces[2].astype(jnp.bfloat16)
    outputs = lax.map(attend_head, (query_rows, key_rows, value_rows))
    joined = outputs.transpose(1, 2, 0, 3).reshape(batch_count * length, heads * HEAD_SIZE)
    attention = jnp.dot(joined, out_weight, preferred_element_type=jnp.float32).reshape(batch_count, length, width)
    summed = tokens.astype(jnp.float32) + attention
    return summed * inverse_rms(summed) * gain_out

def reference(tokens, projections, out_weight, gain_in, gain_out, iterates, images):
    mixed = iterates[0]
    image = images[0]
    for step_index in range(ITERS):
        residuals = images - iterates
        gram = jnp.einsum('mbsd,nbsd->mn', residuals, residuals, precision=lax.Precision.HIGHEST)
        alpha = anderson_weights(gram)
        mixed = jnp.einsum('m,mbsd->bsd', alpha, images, precision=lax.Precision.HIGHEST)
        image = layer_map(mixed, tokens, projections, out_weight, gain_in, gain_out)
        iterates = jnp.concatenate([iterates[1:], mixed[None]], axis=0)
        images = jnp.concatenate([images[1:], image[None]], axis=0)
    return (mixed, image)
```

```python
import functools

import jax
import jax.numpy as jnp
import numpy as np
from jax import lax
from jax.experimental import pallas as pl
from jax.experimental.pallas import tpu as pltpu
from jax.sharding import PartitionSpec as P

HEAD_SIZE = 128
ITERS = 2
MESH = pl.DeviceIdType.MESH

epsilon = 1e-05
rope_base = 10000.0
ridge_factor = 0.01

LANES = 128

f32 = jnp.float32
bf16 = jnp.bfloat16


def rope_tables(length):
    half = HEAD_SIZE // 2
    frequency = rope_base ** (-2.0 * np.arange(half) / HEAD_SIZE)
    angles = np.arange(length)[:, None] * frequency[None, :]
    cosine, sine = np.cos(angles), np.sin(angles)
    return np.stack(
        [np.concatenate([cosine, cosine], 1), np.concatenate([-sine, sine], 1)]
    ).astype(np.float32)


def anderson_weights(gram):
    extent = len(gram)
    trace = gram[0][0]
    for m in range(1, extent):
        trace = trace + gram[m][m]
    ridge = ridge_factor * trace / extent
    matrix = [[gram[m][n] + ridge if m == n else gram[m][n] for n in range(extent)] for m in range(extent)]
    target = [jnp.ones_like(ridge) for _ in range(extent)]
    for column in range(extent):
        for row in range(column + 1, extent):
            factor = matrix[row][column] / matrix[column][column]
            for k in range(column + 1, extent):
                matrix[row][k] = matrix[row][k] - factor * matrix[column][k]
            target[row] = target[row] - factor * target[column]
    answer = [None] * extent
    for column in reversed(range(extent)):
        value = target[column]
        for k in range(column + 1, extent):
            value = value - matrix[column][k] * answer[k]
        answer[column] = value / matrix[column][column]
    total = answer[0]
    for m in range(1, extent):
        total = total + answer[m]
    return [a / total for a in answer]


def swaps_heads(n_seq, heads):
    return heads % n_seq == 0 and n_seq & (n_seq - 1) == 0


def kernel(
    n_seq, n_tp,
    tokens, proj_hbm, out_hbm, gain_in, gain_out, iterates, images, rope_hbm,
    mixed_out, image_out,
    proj, out_w, rope, xbuf, acc, kv, qbuf, att, psend, precv, zsend, zrecv,
    summed, colbuf, tp_stat, seq_stat, stage, piece,
    load_sem, tp_send, tp_recv, seq_send, seq_recv, x_send, x_recv, r_send, r_recv,
    kv_send, kv_recv, p_send, p_recv, z_send, z_recv, o_send, o_recv,
):
    mem, length, width = images.shape
    embed = acc.shape[2]
    heads = embed // HEAD_SIZE
    swap = swaps_heads(n_seq, heads)
    n_z = n_tp // 2
    full_width = n_tp * width
    seq = lax.axis_index("seq")
    tp = lax.axis_index("tp")
    core = lax.rem(tp, 2)
    z = lax.div(tp, 2)
    partner = z * 2 + 1 - core
    CH = 16
    chunks = length // CH
    lane = lax.broadcasted_iota(jnp.int32, (CH, 128), 1)
    pending = []

    loads = [
        pltpu.make_async_copy(proj_hbm, proj, load_sem.at[0]),
        pltpu.make_async_copy(out_hbm, out_w, load_sem.at[1]),
        pltpu.make_async_copy(
            rope_hbm.at[:, pl.ds(pl.multiple_of(seq * length, 128), length), :], rope, load_sem.at[2]
        ),
    ]
    for load in loads:
        load.start()

    barrier = pltpu.get_barrier_semaphore()
    for d in range(1, n_tp):
        pl.semaphore_signal(barrier, inc=1, device_id={"tp": lax.rem(tp + d, n_tp)}, device_id_type=MESH)
    for d in range(1, n_seq):
        pl.semaphore_signal(barrier, inc=1, device_id={"seq": lax.rem(seq + d, n_seq)}, device_id_type=MESH)

    def remote(src, dst, send, recv, device):
        return pltpu.make_async_remote_copy(
            src_ref=src, dst_ref=dst, send_sem=send, recv_sem=recv, device_id=device, device_id_type=MESH
        )

    def post(buf, sends, recvs, phase, axis, me, n, count):
        copies = []
        rows = pl.ds(0, count)
        for d in range(1, n):
            copy = remote(
                buf.at[phase, me, rows], buf.at[phase, me, rows], sends.at[phase, d], recvs.at[phase, d],
                {axis: lax.rem(me + d, n)},
            )
            copy.start()
            copies.append(copy)
        pending.extend(copies)
        return copies

    def collect(buf, copies, phase, n, count=1):
        for copy in copies:
            copy.wait_recv()
        total = buf[phase, 0, :count]
        for j in range(1, n):
            total = total + buf[phase, j, :count]
        return total

    def post_tp(phase, count=1):
        return post(tp_stat, tp_send, tp_recv, phase, "tp", tp, n_tp, count)

    def post_seq(phase, count=1):
        return post(seq_stat, seq_send, seq_recv, phase, "seq", seq, n_seq, count)

    pairs = [(m, n) for m in range(mem) for n in range(m, mem)]

    def gram_step(i, sums):
        rows = pl.ds(pl.multiple_of(i * 8, 8), 8)
        res = [images[m, rows, :] - iterates[m, rows, :] for m in range(mem)]
        out = []
        for (m, n), total in zip(pairs, sums):
            product = res[m] * res[n]
            for c in range(width // 128):
                total = total + product[:, c * 128:(c + 1) * 128]
            out.append(total)
        return tuple(out)

    sums = lax.fori_loop(0, length // 8, gram_step, tuple(jnp.zeros((8, 128), f32) for _ in pairs))
    def packed(totals):
        rows = [jnp.sum(total, axis=0, keepdims=True) for total in totals]
        block = jnp.concatenate(rows + [jnp.zeros((LANES - len(rows), LANES), f32)], axis=0)
        return jnp.sum(jnp.transpose(block), axis=0, keepdims=True)

    def unpacked(row):
        return jnp.transpose(jnp.broadcast_to(row, (LANES, LANES)))

    tp_stat[0, tp, :1] = packed(sums)

    if not swap:
        for it in range(ITERS):
            for j in range(1, n_seq):
                @pl.when(j > seq)
                def _():
                    kv[it, :, j, 1] = jnp.zeros((heads, length, HEAD_SIZE), bf16)

    pl.semaphore_wait(barrier, n_tp - 1 + n_seq - 1)

    seq_stat[0, seq, :1] = collect(tp_stat, post_tp(0), 0, n_tp)
    entries = unpacked(collect(seq_stat, post_seq(0), 0, n_seq))

    gram = [[None] * mem for _ in range(mem)]
    for p, (m, n) in enumerate(pairs):
        gram[m][n] = gram[n][m] = entries[p:p + 1, :]

    halves = xbuf.shape[2]
    part = width // halves
    steps = (1, -1)

    def inside(place):
        return jnp.logical_and(place >= 0, place < n_z)

    def guarded(condition, act):
        @pl.when(condition)
        def _():
            act()

    share = heads // n_seq

    def peer(j):
        place = 0
        bit = 1
        while bit < n_seq:
            place = place + lax.rem(lax.div(seq, bit) + (j // bit) % 2, 2) * bit
            bit *= 2
        return place

    def swap_copy(it, j, c):
        return remote(
            stage.at[it, j, c], kv.at[it, c, :, seq], kv_send.at[it, j, c], kv_recv.at[it, j, c], {"seq": peer(j)}
        )

    def back_copy(it, i):
        cols = pl.ds(pl.multiple_of(seq * share * HEAD_SIZE, HEAD_SIZE), share * HEAD_SIZE)
        return remote(piece.at[it, i], att.at[it, :, cols], o_send.at[it, i], o_recv.at[it, seq], {"seq": i})

    def back_arrival(it, i):
        cols = slice(i * share * HEAD_SIZE, (i + 1) * share * HEAD_SIZE)
        return remote(piece.at[it, i], att.at[it, :, cols], o_send.at[it, i], o_recv.at[it, i], {"seq": i})

    def exchange(it, rotated, row_scale):
        def shaped(c, cols):
            return (acc[c, :, cols] * row_scale).astype(bf16) if c == 2 else rotated(c, cols)

        for c in (2, 1, 0):
            for j in reversed(range(1, n_seq)):
                for g in range(share):
                    cols = pl.ds(pl.multiple_of((peer(j) * share + g) * HEAD_SIZE, HEAD_SIZE), HEAD_SIZE)
                    stage[it, j, c, g] = shaped(c, cols)
                swap_copy(it, j, c).start()
        for c in (2, 1, 0):
            for g in range(share):
                cols = pl.ds(pl.multiple_of((seq * share + g) * HEAD_SIZE, HEAD_SIZE), HEAD_SIZE)
                kv[it, c, g, seq] = shaped(c, cols)
        for c in (2, 1, 0):
            for j in reversed(range(1, n_seq)):
                swap_copy(it, j, c).wait_recv()
        for i in range(n_seq):
            count = (i + 1) * length
            query_index = i * length + lax.broadcasted_iota(jnp.int32, (length, count), 0)
            allowed = lax.broadcasted_iota(jnp.int32, (length, count), 1) <= query_index
            for g in range(share):
                keys = kv[it, 1, g, :i + 1].reshape(count, HEAD_SIZE)
                values = kv[it, 2, g, :i + 1].reshape(count, HEAD_SIZE)
                scores = lax.dot_general(
                    kv[it, 0, g, i], keys, (((1,), (1,)), ((), ())), preferred_element_type=f32
                ) * HEAD_SIZE ** (-0.5)
                scores = jnp.where(allowed, scores, -1e30)
                weights = jnp.where(allowed, jnp.exp(scores - jnp.max(scores, axis=1, keepdims=True)), 0.0)
                total = jnp.sum(weights, axis=1, keepdims=True)
                mixture = jnp.dot(weights.astype(bf16), values, preferred_element_type=f32)
                piece[it, i, :, g * HEAD_SIZE:(g + 1) * HEAD_SIZE] = (mixture / total).astype(bf16)

            @pl.when(seq == i)
            def _():
                att[it, :, i * share * HEAD_SIZE:(i + 1) * share * HEAD_SIZE] = piece[it, i]

            guarded(seq != i, back_copy(it, i).start)
        for i in range(n_seq):
            guarded(seq != i, back_arrival(it, i).wait_recv)

    for it in range(ITERS):
        last = it + 1 == ITERS
        alpha = anderson_weights(gram)
        groups = width // LANES

        def mix_step(i, sums):
            rows = pl.ds(pl.multiple_of(i * CH, CH), CH)
            squares = None
            sums = list(sums)
            for c in range(groups):
                cols = slice(c * LANES, (c + 1) * LANES)
                stored = [images[m, rows, cols] for m in range(it, mem)] + ([image_out[rows, cols]] if it else [])
                mixed = alpha[0] * stored[0]
                for m in range(1, mem):
                    mixed = mixed + alpha[m] * stored[m]
                mixed_out[rows, cols] = mixed
                ready = (mixed * gain_in[:, cols]).astype(bf16)
                xbuf[it, tp, c * LANES // part, rows, c * LANES % part:c * LANES % part + LANES] = ready
                square = mixed * mixed
                squares = square if squares is None else squares + square
                if not last:
                    for m in range(1, mem):
                        sums[m - 1] = sums[m - 1] + mixed * (images[m, rows, cols] - iterates[m, rows, cols])
            if not last:
                sums[mem - 1] = sums[mem - 1] + squares
            colbuf[rows, :] = squares
            return tuple(sums)

        fixed = lax.fori_loop(
            0, chunks, mix_step, () if last else tuple(jnp.zeros((CH, LANES), f32) for _ in range(mem))
        )

        def x_copy(side, k, q):
            slot = (z - steps[side] * (k - 1)) * 2 + core
            return remote(
                xbuf.at[it, slot, q], xbuf.at[it, slot, q], x_send.at[it, side, k, q], x_recv.at[it, side, k, q],
                {"tp": (z + steps[side]) * 2 + core},
            )

        def x_arrival(side, k, q):
            slot = (z - steps[side] * k) * 2 + core
            return remote(
                xbuf.at[it, slot, q], xbuf.at[it, slot, q], x_send.at[it, side, k, q], x_recv.at[it, side, k, q],
                {"tp": partner},
            )

        def relay(side, k, q):
            slot = (z - steps[side] * k) * 2 + core
            return remote(
                xbuf.at[it, slot, q], xbuf.at[it, slot, q], r_send.at[it, side, k, q], r_recv.at[it, side, k, q],
                {"tp": partner},
            )

        def project(slot, q):
            rows = pl.ds(pl.multiple_of(slot * width + q * part, 128), part)
            for c in range(3):
                acc[c] += jnp.dot(xbuf[it, slot, q], proj[c, rows, :], preferred_element_type=f32)

        for q in range(halves):
            for side in range(2):
                guarded(inside(z + steps[side]), x_copy(side, 1, q).start)
        for q in range(halves):
            relay(0, 0, q).start()
        tp_stat[1 + 2 * it, tp, :1] = jnp.sum(jnp.transpose(colbuf[...]), axis=0, keepdims=True)
        if not last:
            tp_stat[1 + 2 * it, tp, 1:2] = packed(fixed)
        square_copies = post_tp(1 + 2 * it, 1 if last else 2)
        if it == 0:
            loads[0].wait()
        acc[...] = jnp.zeros(acc.shape, f32)
        for q in range(halves):
            project(tp, q)
        for q in range(halves):
            relay(0, 0, q).wait_recv()
            project(partner, q)

        def arrive(side, k, q):
            x_arrival(side, k, q).wait_recv()
            if k + 1 < n_z:
                guarded(inside(z + steps[side]), x_copy(side, k + 1, q).start)
            relay(side, k, q).start()

        def across(side, k, q):
            relay(side, k, q).wait_recv()
            project((z - steps[side] * k) * 2 + 1 - core, q)

        for k in range(1, n_z):
            for q in range(halves):
                for side in range(2):
                    guarded(inside(z - steps[side] * k), functools.partial(arrive, side, k, q))
                for side in range(2):
                    guarded(
                        inside(z - steps[side] * k),
                        functools.partial(project, (z - steps[side] * k) * 2 + core, q),
                    )
                for side in range(2):
                    guarded(inside(z - steps[side] * k), functools.partial(across, side, k, q))
        squares = collect(tp_stat, square_copies, 1 + 2 * it, n_tp, 1 if last else 2)
        if not last:
            fixed = unpacked(squares[1:2, :]) * (1.0 / LANES)
            squares = squares[:1, :]
        row_scale = jnp.transpose(
            jnp.broadcast_to(lax.rsqrt(squares / full_width + epsilon), (length, length))
        )
        if it == 0:
            loads[2].wait()
        cosine, sine = rope[0] * row_scale, rope[1] * row_scale

        def rotated(c, cols):
            rows = acc[c, :, cols]
            return (rows * cosine + pltpu.roll(rows, HEAD_SIZE // 2, 1) * sine).astype(bf16)

        kv_copies = [[] for _ in range(heads)]
        if swap:
            exchange(it, rotated, row_scale)
        for h in range(0 if swap else heads):
            cols = slice(h * HEAD_SIZE, (h + 1) * HEAD_SIZE)
            kv[it, h, seq, 0] = rotated(1, cols)
            kv[it, h, seq, 1] = (acc[2, :, cols] * row_scale).astype(bf16)
            for d in reversed(range(1, n_seq)):
                copy = remote(
                    kv.at[it, h, seq], kv.at[it, h, seq], kv_send.at[it, h, d], kv_recv.at[it, h, d],
                    {"seq": lax.rem(seq + d, n_seq)},
                )
                guarded(seq + d < n_seq, copy.start)
                kv_copies[h].append((d, copy))
        for h in range(0 if swap else heads):
            cols = slice(h * HEAD_SIZE, (h + 1) * HEAD_SIZE)
            qbuf[:, cols] = rotated(0, cols)

        total_keys = n_seq * length
        query_index = seq * length + lax.broadcasted_iota(jnp.int32, (length, total_keys), 0)
        allowed = lax.broadcasted_iota(jnp.int32, (length, total_keys), 1) <= query_index
        for h in range(0 if swap else heads):
            cols = slice(h * HEAD_SIZE, (h + 1) * HEAD_SIZE)
            for d, copy in kv_copies[h]:
                guarded(seq >= d, copy.wait_recv)
            keys = kv[it, h, :, 0].reshape(total_keys, HEAD_SIZE)
            values = kv[it, h, :, 1].reshape(total_keys, HEAD_SIZE)
            scores = lax.dot_general(
                qbuf[:, cols], keys, (((1,), (1,)), ((), ())), preferred_element_type=f32
            ) * HEAD_SIZE ** (-0.5)
            scores = jnp.where(allowed, scores, -1e30)
            weights = jnp.where(allowed, jnp.exp(scores - jnp.max(scores, axis=1, keepdims=True)), 0.0)
            total = jnp.sum(weights, axis=1, keepdims=True)
            mixture = jnp.dot(weights.astype(bf16), values, preferred_element_type=f32)
            att[it, :, cols] = (mixture / total).astype(bf16)

        if it == 0:
            loads[1].wait()

        def partial(place, side_core, q):
            cols = pl.ds(pl.multiple_of((place * 2 + side_core) * width + q * part, 128), part)
            return jnp.dot(att[it], out_w[:, cols], preferred_element_type=f32)

        def p_copy(side, k, q):
            return remote(
                psend.at[it, side, k, q], precv.at[it, side, k, q],
                p_send.at[it, side, k, q], p_recv.at[it, side, k, q], {"tp": partner},
            )

        def z_copy(side, k, q):
            return remote(
                zsend.at[it, side, k, q], zrecv.at[it, side, k - 1, q],
                z_send.at[it, side, k, q], z_recv.at[it, side, k - 1, q],
                {"tp": (z + steps[side]) * 2 + core},
            )

        def arrival(side, k, q):
            return remote(
                zsend.at[it, side, k, q], zrecv.at[it, side, k, q],
                z_send.at[it, side, k, q], z_recv.at[it, side, k, q],
                {"tp": partner},
            )

        def give(side, k, q):
            psend[it, side, k, q] = partial(z + steps[side] * k, 1 - core, q).astype(bf16)
            p_copy(side, k, q).start()

        def pass_on(side, k, q):
            own = partial(z + steps[side] * k, core, q)
            p_copy(side, k, q).wait_recv()
            own = own + precv[it, side, k, q].astype(f32)
            if k + 1 < n_z:
                behind = inside(z - steps[side])
                guarded(behind, arrival(side, k, q).wait_recv)
                own = own + jnp.where(behind, zrecv[it, side, k, q].astype(f32), 0.0)
            zsend[it, side, k, q] = own.astype(bf16)
            z_copy(side, k, q).start()

        order = [(k, q) for k in reversed(range(1, n_z)) for q in range(halves)]
        offers = order + [(0, q) for q in range(halves)]
        ahead = 2 * halves

        def offer(k, q):
            if k == 0:
                give(0, 0, q)
            else:
                for side in range(2):
                    guarded(inside(z + steps[side] * k), functools.partial(give, side, k, q))

        for k, q in offers[:ahead]:
            offer(k, q)
        for i, (k, q) in enumerate(order):
            for side in range(2):
                guarded(inside(z + steps[side] * k), functools.partial(pass_on, side, k, q))
            if ahead + i < len(offers):
                offer(*offers[ahead + i])
        for k, q in offers[ahead + len(order):]:
            offer(k, q)
        for q in range(halves):
            cols = slice(q * part, (q + 1) * part)
            own = partial(z, core, q) + tokens[:, cols].astype(f32)
            p_copy(0, 0, q).wait_recv()
            summed[:, cols] = own + precv[it, 0, 0, q].astype(f32)
        for q in range(halves):
            cols = slice(q * part, (q + 1) * part)
            for side in range(2):
                def take(side=side, q=q, cols=cols):
                    arrival(side, 0, q).wait_recv()
                    summed[:, cols] += zrecv[it, side, 0, q].astype(f32)

                guarded(inside(z - steps[side]), take)

        def sum_step(i, carry):
            rows = pl.ds(pl.multiple_of(i * CH, CH), CH)
            layer = summed[rows, :]
            scaled = layer * gain_out[...]
            summed[rows, :] = scaled
            stats = [layer * layer]
            if not last:
                stats += [scaled * (images[m, rows, :] - iterates[m, rows, :]) for m in range(1, mem)]
                stats += [scaled * scaled, scaled * mixed_out[rows, :]]
            columns = jnp.zeros((CH, 128), f32)
            for k, stat in enumerate(stats):
                columns = jnp.where(lane == k, jnp.sum(stat, axis=1, keepdims=True), columns)
            colbuf[rows, :] = columns
            return carry

        lax.fori_loop(0, chunks, sum_step, 0)
        count = 1 if last else mem + 2
        tp_stat[2 + 2 * it, tp, :count] = jnp.transpose(colbuf[...])[:count, :]
        stats = collect(tp_stat, post_tp(2 + 2 * it, count), 2 + 2 * it, n_tp, count)
        scale_row = lax.rsqrt(stats[:1, :] / full_width + epsilon)

        if not last:
            seq_stat[1, seq, :mem - 1] = scale_row * stats[1:mem, :] - fixed[:mem - 1, :]
            seq_stat[1, seq, mem - 1:mem] = (
                scale_row * scale_row * stats[mem:mem + 1, :]
                - 2.0 * scale_row * stats[mem + 1:mem + 2, :]
                + fixed[mem - 1:mem, :]
            )
            seq_copies = post_seq(1, mem)
        scale_cols = jnp.transpose(jnp.broadcast_to(scale_row, (length, length)))
        for c in range(width // 128):
            cols = slice(c * 128, (c + 1) * 128)
            image_out[:, cols] = summed[:, cols] * scale_cols
        if not last:
            new = collect(seq_stat, seq_copies, 1, n_seq, mem)
            new = jnp.broadcast_to(jnp.sum(new, axis=1, keepdims=True), new.shape)
            grown = [[None] * mem for _ in range(mem)]
            for m in range(mem - 1):
                for n in range(mem - 1):
                    grown[m][n] = gram[m + 1][n + 1]
                grown[m][mem - 1] = grown[mem - 1][m] = new[m:m + 1, :]
            grown[mem - 1][mem - 1] = new[mem - 1:mem, :]
            gram = grown

        for h in range(heads):
            for d, copy in kv_copies[h]:
                guarded(seq + d < n_seq, copy.wait_send)
        if swap:
            for j in range(1, n_seq):
                for c in range(3):
                    swap_copy(it, j, c).wait_send()
            for i in range(n_seq):
                guarded(seq != i, back_copy(it, i).wait_send)
        for q in range(halves):
            relay(0, 0, q).wait_send()
            p_copy(0, 0, q).wait_send()
            for side in range(2):
                for k in range(1, n_z):
                    guarded(
                        jnp.logical_and(inside(z + steps[side]), inside(z - steps[side] * (k - 1))),
                        x_copy(side, k, q).wait_send,
                    )
                    guarded(inside(z - steps[side] * k), relay(side, k, q).wait_send)
                    guarded(inside(z + steps[side] * k), p_copy(side, k, q).wait_send)
                    guarded(inside(z + steps[side] * k), z_copy(side, k, q).wait_send)

    for copy in pending:
        copy.wait_send()


def solution(mesh):
    n_seq, n_tp = mesh.shape["seq"], mesh.shape["tp"]

    def shards(tokens, projections, out_weight, gain_in, gain_out, iterates, images):
        batch, length, width = tokens.shape
        mem = images.shape[0]
        embed = projections.shape[2]
        n_z = n_tp // 2
        heads = embed // HEAD_SIZE
        halves = 2 if width % 256 == 0 else 1
        part = width // halves
        swap = swaps_heads(n_seq, heads)
        share = max(heads // n_seq, 1)
        if swap:
            kv_shape = (ITERS, 3, share, n_seq, length, HEAD_SIZE)
            kv_sems = (ITERS, n_seq, 3)
            stage_shape = (ITERS, n_seq, 3, share, length, HEAD_SIZE)
            piece_shape = (ITERS, n_seq, length, share * HEAD_SIZE)
            query_shape = (8, 128)
        else:
            kv_shape = (ITERS, heads, n_seq, 2, length, HEAD_SIZE)
            kv_sems = (ITERS, heads, n_seq)
            stage_shape = piece_shape = (8, 128)
            query_shape = (length, embed)
        vmem = pl.BlockSpec(memory_space=pltpu.VMEM)
        hbm = pl.BlockSpec(memory_space=pl.ANY)
        dma = pltpu.SemaphoreType.DMA
        out = jax.ShapeDtypeStruct((length, width), f32)
        mixed, image = pl.pallas_call(
            functools.partial(kernel, n_seq, n_tp),
            out_shape=(out, out),
            in_specs=[vmem, hbm, hbm, vmem, vmem, vmem, vmem, hbm],
            out_specs=(vmem, vmem),
            scratch_shapes=[
                pltpu.VMEM((3, n_tp * width, embed), bf16),
                pltpu.VMEM((embed, n_tp * width), bf16),
                pltpu.VMEM((2, length, HEAD_SIZE), f32),
                pltpu.VMEM((ITERS, n_tp, halves, length, part), bf16),
                pltpu.VMEM((3, length, embed), f32),
                pltpu.VMEM(kv_shape, bf16),
                pltpu.VMEM(query_shape, bf16),
                pltpu.VMEM((ITERS, length, embed), bf16),
                pltpu.VMEM((ITERS, 2, n_z, halves, length, part), bf16),
                pltpu.VMEM((ITERS, 2, n_z, halves, length, part), bf16),
                pltpu.VMEM((ITERS, 2, n_z, halves, length, part), bf16),
                pltpu.VMEM((ITERS, 2, n_z, halves, length, part), bf16),
                pltpu.VMEM((length, width), f32),
                pltpu.VMEM((length, 128), f32),
                pltpu.VMEM((1 + 2 * ITERS, n_tp, 8, 128), f32),
                pltpu.VMEM((ITERS, n_seq, 8, 128), f32),
                pltpu.VMEM(stage_shape, bf16),
                pltpu.VMEM(piece_shape, bf16),
                dma((3,)),
                dma((1 + 2 * ITERS, n_tp)), dma((1 + 2 * ITERS, n_tp)),
                dma((ITERS, n_seq)), dma((ITERS, n_seq)),
                dma((ITERS, 2, n_z, halves)), dma((ITERS, 2, n_z, halves)),
                dma((ITERS, 2, n_z, halves)), dma((ITERS, 2, n_z, halves)),
                dma(kv_sems), dma(kv_sems),
                dma((ITERS, 2, n_z, halves)), dma((ITERS, 2, n_z, halves)),
                dma((ITERS, 2, n_z, halves)), dma((ITERS, 2, n_z, halves)),
                dma((ITERS, n_seq)), dma((ITERS, n_seq)),
            ],
            compiler_params=pltpu.CompilerParams(
                collective_id=0, has_side_effects=True, vmem_limit_bytes=60 * 1024 * 1024
            ),
            name="anderson_layer",
        )(
            tokens.reshape(length, width),
            projections.transpose(1, 0, 2),
            out_weight,
            gain_in.reshape(1, width),
            gain_out.reshape(1, width),
            iterates.reshape(mem, length, width),
            images.reshape(mem, length, width),
            jnp.asarray(rope_tables(n_seq * length)),
        )
        return mixed.reshape(batch, length, width), image.reshape(batch, length, width)

    in_specs = (
        P(None, "seq", "tp"),
        P(None, None, "tp"),
        P("tp", None),
        P("tp"),
        P("tp"),
        P(None, None, "seq", "tp"),
        P(None, None, "seq", "tp"),
    )
    out_specs = (P(None, "seq", "tp"), P(None, "seq", "tp"))
    return jax.shard_map(shards, mesh=mesh, in_specs=in_specs, out_specs=out_specs, check_vma=False)
```
